32 devices in a mesh: sub: 8 (over z, y), panel: 4 (over x, core).
Axes of the slice: x: 2, y: 2, z: 4, core: 2. Of those that a mesh axis runs over, the one named last changes fastest.
Arguments:
- interior_factor: float32 [64, 512, 512], P('sub'), may hold values from -1 to 3, as said below
- coupling: bfloat16 [64, 512, 2048], P('sub', None, 'panel'), may hold values from -1 to 1
- interface_diag: float32 [8192], P(('sub', 'panel')), may hold values from 0.5 to 4
- interface_column: float32 [8192, 128], P(('sub', 'panel')), may hold values from -1.8 to 1.8
- block_map: int32 [64, 16], replicated, may hold values from 0 to 63, as said below
- pair_pattern: int32 [64, 8], P('sub'), may hold values 0 or 1
Outputs:
- assembled: float32 [8192, 1024], P(('sub', 'panel'))
- factored: float32 [8192, 1024], P(('sub', 'panel'))
The draws below stay inside these ranges and needn't reach their ends.
Inputs may be any that keep to these rules, and one draw needn't show every extreme that they name: Local block a of a subdomain has its owner block_map // 8 and its position block_map % 8 among that owner's blocks, one of the 2 positions from (a // 4) * 2. Blocks a and b of one subdomain with a % 4 == b % 4 have the same owner. The 32 block groups of the subdomains of one index of sub go at most 4 to one owner, and some owner gets exactly 4 of them. `interior_factor`: lower triangular; the diagonal lies between 1 and 3.
All inputs are finite; a program needn't handle non-finite values. No bound on the sum of `pair_pattern` on one device may be relied on, other than what follows from the above.
Results may differ from the reference program's by a relative error of at most 0.0006.
Values may be sent and summed in bfloat16 or wider, within the bound.
A program may use at most 128 MiB of HBM per device.

```python
import math
import jax
import jax.numpy as jnp
from jax import lax

BLK = 128
NS = 2048
NIN = 512
SUB_DEV = 8
OWN = 8
NLOC = 16
GRP = 4
R = 2
RPO = 4
SUBDOMAINS = 64
NBLK = 64
N_SUB = 8
N_PANEL = 4


def draw_interior_factor(key, part):
    key_diag, key_lower = jax.random.split(jax.random.fold_in(key, 7))
    diagonal = jnp.exp(jax.random.uniform(key_diag, (SUBDOMAINS, NIN), jnp.float32, 0.0, math.log(2.0)))
    lower = 1.5 * jnp.clip(jax.random.normal(key_lower, (SUBDOMAINS, NIN, NIN), jnp.float32), -3.5, 3.5)
    strict = jnp.tril(lower, -1) / math.sqrt(NIN)
    return strict + diagonal[:, :, None] * jnp.eye(NIN, dtype=jnp.float32)[None]


def draw_coupling(key, part):
    key_base, key_shift = jax.random.split(jax.random.fold_in(key, 11))
    base = jnp.clip(jax.random.normal(key_base, (SUBDOMAINS, NIN, NS), jnp.float32), -3.0, 3.0)
    shift = 0.25 * jnp.clip(jax.random.normal(key_shift, (SUBDOMAINS, NIN, 1), jnp.float32), -3.0, 3.0)
    return ((base + shift) / math.sqrt(NIN)).astype(jnp.bfloat16)


def draw_block_map(key, part):
    key_rank, key_noise, key_order, key_rows = jax.random.split(jax.random.fold_in(key, 23), 4)
    item_total = N_SUB * RPO
    popularity = jax.random.permutation(key_rank, N_SUB).astype(jnp.int32)
    owner_of_item = jnp.arange(item_total, dtype=jnp.int32) // RPO
    noise = jax.random.randint(key_noise, (N_SUB, item_total), 0, 1024, dtype=jnp.int32)
    score = noise + popularity[owner_of_item][None, :] * (2048 // N_SUB)
    distinct = score * item_total + jnp.arange(item_total, dtype=jnp.int32)[None, :]
    chosen = lax.top_k(distinct, GRP * SUB_DEV)[1].astype(jnp.int32)
    shuffle = jax.vmap(lambda sub_key: jax.random.permutation(sub_key, GRP * SUB_DEV))(jax.random.split(key_order, N_SUB))
    chosen = jnp.take_along_axis(chosen, shuffle.astype(jnp.int32), axis=1)
    owners = owner_of_item[chosen].reshape(SUBDOMAINS, GRP)
    rows = jax.random.randint(key_rows, (SUBDOMAINS, N_PANEL, GRP), 0, R, dtype=jnp.int32)
    panels = jnp.arange(N_PANEL, dtype=jnp.int32)[None, :, None]
    blocks = owners[:, None, :] * OWN + panels * R + rows
    return blocks.reshape(SUBDOMAINS, N_PANEL * GRP)


def set_ends(drawn, key, least, high):
    longest = drawn.shape.index(max(drawn.shape))
    spots = []
    for shift in (0, 1):
        where = [jax.random.randint(jax.random.fold_in(key, axis), (), 0, length) for axis, length in enumerate(drawn.shape)]
        where[longest] = (where[longest] + shift) % drawn.shape[longest]
        spots.append(tuple(where))
    return drawn.at[spots[0]].set(least).at[spots[1]].set(high)


def steps_of(stream_key, extent, pieces, least, high):
    def one(position, shards_of):
        draws = jax.random.uniform(jax.random.fold_in(jax.random.fold_in(stream_key, 6), position), (shards_of,), jnp.float32, least / len(pieces), high / len(pieces))
        return jnp.repeat(jnp.exp(draws), extent[position] // shards_of).reshape((-1,) + (1,) * (len(extent) - position - 1))

    gain = one(*pieces[0])
    for cut in pieces[1:]:
        gain = gain * one(*cut)
    return gain


def scatter_about(key, extent, width, most, pieces=(), kind=jnp.bfloat16):
    drawn = width * jax.random.normal(key, extent, jnp.float32)
    if pieces:
        drawn = drawn * steps_of(key, extent, pieces, -0.22, 0.18)
    return jnp.clip(drawn, -most, most).astype(kind)


def setup_inputs(seed: int = 0) -> dict:
    splits = jax.random.split(jax.random.key(seed), 7)
    interior_factor = draw_interior_factor(jax.random.fold_in(splits[6], 71), 0)
    coupling = draw_coupling(jax.random.fold_in(splits[6], 71), 0)
    interface_diag = jnp.clip(jnp.exp(math.log(4.0) - 2.0794415 * jax.random.uniform(splits[2], (NBLK * BLK,), jnp.float32) ** steps_of(splits[2], (NBLK * BLK,), ((0, 32),), -0.2, 0.2)), 0.5, 4.0)
    interface_column = scatter_about(splits[3], (NBLK * BLK, BLK), 0.3, 1.8, ((0, 32),), jnp.float32)
    block_map = draw_block_map(jax.random.fold_in(splits[6], 71), 0)
    pair_pattern = set_ends((jax.random.randint(splits[5], (SUBDOMAINS, NLOC // 2), 0, 4) < 3).astype(jnp.int32), jax.random.fold_in(splits[5], 1), 0, 1)
    return {"interior_factor": interior_factor, "coupling": coupling, "interface_diag": interface_diag, "interface_column": interface_column, "block_map": block_map, "pair_pattern": pair_pattern}


def local_tiles(factor, couple, pattern):
    solved = lax.linalg.triangular_solve(factor, couple.astype(jnp.float32), left_side=True, lower=True)
    rounded = lax.optimization_barrier(solved.astype(jnp.bfloat16))
    blocks = rounded.astype(jnp.float32).reshape(NIN, NLOC, BLK)
    partner = jnp.roll(blocks, -(NLOC // 2), axis=1)
    diagonal = jnp.einsum('kai,kaj->aij', blocks, blocks)
    cross_tiles = jnp.einsum('kai,kaj->aij', blocks, partner)
    linked = jnp.concatenate([pattern, pattern]).astype(jnp.float32)
    return (diagonal, cross_tiles * linked[:, None, None])

def factor_step(square):
    column = square[:, :BLK]
    pivot = jnp.linalg.cholesky(column[:BLK])
    solved = lax.linalg.triangular_solve(pivot, column.T, left_side=True, lower=True).T
    lower_col = jnp.concatenate([pivot, solved[BLK:]], axis=0)
    update = jnp.dot(lower_col, lower_col.T, precision=lax.Precision.HIGHEST)
    row_ids = jnp.arange(square.shape[0], dtype=jnp.int32)[:, None]
    updated = jnp.where(row_ids < BLK, square, square - update)
    return jnp.concatenate([lower_col, updated[:, BLK:]], axis=1)

def reference(interior_factor, coupling, interface_diag, interface_column, block_map, pair_pattern):

    def add_one(total, items):
        factor, couple, blocks, pattern = items
        diagonal, cross_tiles = local_tiles(factor, couple, pattern)
        partner_blocks = jnp.roll(blocks, -(NLOC // 2))
        total = total.at[blocks, blocks % OWN].add(diagonal)
        total = total.at[blocks, partner_blocks % OWN].add(cross_tiles)
        return (total, None)
    start = jnp.zeros((NBLK, OWN, BLK, BLK), jnp.float32)
    total, unused = lax.scan(add_one, start, (interior_factor, coupling, block_map, pair_pattern))
    diag_values = interface_diag.reshape(NBLK, BLK)
    identity = jnp.eye(BLK, dtype=jnp.float32)
    index = jnp.arange(NBLK, dtype=jnp.int32)
    total = total.at[index, index % OWN].add(diag_values[:, :, None] * identity[None])
    off_pivot = (index % OWN != 0).astype(jnp.float32)
    column_tiles = interface_column.reshape(NBLK, BLK, BLK) * off_pivot[:, None, None]
    total = total.at[:, 0].add(column_tiles)
    assembled = total.transpose(0, 2, 1, 3).reshape(NBLK * BLK, OWN * BLK)
    squares = assembled.reshape(N_SUB, OWN * BLK, OWN * BLK)
    factored = lax.map(factor_step, squares)
    return (assembled, factored.reshape(NBLK * BLK, OWN * BLK))
```

```python
import jax
import jax.numpy as jnp
from jax import lax
from jax.experimental import pallas as pl
from jax.experimental.pallas import tpu as pltpu
from jax.sharding import PartitionSpec as P

BLK = 128
OWN = 8
BASE = 32
EXTRA = 16
F32 = jnp.float32
BF16 = jnp.bfloat16
VMEM_LIMIT = 60 * 1024 * 1024


def halves(value):
    high = value.astype(BF16)
    return high, (value - high.astype(F32)).astype(BF16)


def mm(left, right):
    return jnp.dot(left, right, preferred_element_type=F32)


def mm_split(left, right):
    lh, ll = left
    rh, rl = right
    return mm(lh, rh) + (mm(lh, rl) + mm(ll, rh))


def iotas(rows, cols):
    return (
        lax.broadcasted_iota(jnp.int32, (rows, cols), 0),
        lax.broadcasted_iota(jnp.int32, (rows, cols), 1),
    )


def diagonal_inverse(block):
    row8, lane8 = iotas(8, BLK)
    group8 = lane8 // BASE
    within8 = lane8 - group8 * BASE
    tiles = BASE // 8
    rows, cols = iotas(BLK, BLK)
    side = []
    for tile in range(tiles):
        total = jnp.zeros((8, BLK), F32)
        for part in range(BLK // BASE):
            first = part * BASE + tile * 8
            total = jnp.where(group8 == part, block[first : first + 8, :], total)
        side.append(total)
    inverse = [jnp.where(within8 == row8 + tile * 8, 1.0, 0.0).astype(F32) for tile in range(tiles)]
    for step in range(BASE):
        at = step // 8
        inner = step % 8
        lanes = group8 * BASE + step
        spread = {
            tile: jnp.take_along_axis(side[tile], lanes, axis=1, mode="promise_in_bounds")
            for tile in range(at, tiles)
        }
        pivot_row = inverse[at][inner : inner + 1, :] / spread[at][inner : inner + 1, :]
        solved = jnp.broadcast_to(pivot_row, (8, BLK))
        lower = jnp.where(row8 > inner, inverse[at] - spread[at] * solved, inverse[at])
        inverse[at] = jnp.where(row8 == inner, solved, lower)
        for tile in range(at + 1, tiles):
            inverse[tile] = inverse[tile] - spread[tile] * solved
    stacked = jnp.concatenate(inverse * (BLK // BASE), axis=0)
    whole = jnp.where(rows // BASE == cols // BASE, stacked, 0.0)
    size = BASE
    while size < BLK:
        pair = 2 * size
        off = jnp.logical_and(
            rows // pair == cols // pair,
            jnp.logical_and(rows % pair >= size, cols % pair < size),
        )
        split = halves(whole)
        inner_product = mm_split(halves(jnp.where(off, block, 0.0)), split)
        whole = whole - mm_split(split, halves(inner_product))
        size = pair
    return whole


def solve_kernel(half_ref, factor_ref, couple_ref, out_ref, rest_ref):
    count, interior, width = couple_ref.shape
    total = interior // BLK
    inverses = [
        [
            halves(diagonal_inverse(factor_ref[item, b * BLK : (b + 1) * BLK, b * BLK : (b + 1) * BLK]))
            for b in range(total)
        ]
        for item in range(count)
    ]
    for b in range(total):
        for item in range(count):
            low = b * BLK
            inv_high, inv_low = inverses[item][b]
            if b == 0:
                right = couple_ref[item, 0:BLK, :]
                solved = mm(inv_high, right) + mm(inv_low, right)
            else:
                right = halves(rest_ref[item, low : low + BLK, :])
                solved = mm_split((inv_high, inv_low), right)
            out_ref[item, low : low + BLK, :] = solved.astype(BF16)
            if b + 1 < total:
                strip = halves(factor_ref[item, low + BLK :, low : low + BLK])
                update = mm_split(strip, halves(solved))
                if b == 0:
                    before = couple_ref[item, low + BLK :, :].astype(F32)
                else:
                    before = rest_ref[item, low + BLK :, :]
                rest_ref[item, low + BLK :, :] = before - update


def solve_half(half, factor, couple):
    sub_local, interior, width = couple.shape
    number = sub_local // 2
    step = 2 if number % 2 == 0 else 1
    steps = number // step
    return pl.pallas_call(
        solve_kernel,
        grid_spec=pltpu.PrefetchScalarGridSpec(
            num_scalar_prefetch=1,
            grid=(steps,),
            in_specs=[
                pl.BlockSpec((step, interior, interior), lambda i, half: (half[0] * steps + i, 0, 0)),
                pl.BlockSpec((step, interior, width), lambda i, half: (half[0] * steps + i, 0, 0)),
            ],
            out_specs=pl.BlockSpec((step, interior, width), lambda i, half: (i, 0, 0)),
            scratch_shapes=[pltpu.VMEM((step, interior, width), F32)],
        ),
        out_shape=jax.ShapeDtypeStruct((number, interior, width), BF16),
        compiler_params=pltpu.CompilerParams(vmem_limit_bytes=VMEM_LIMIT),
        cost_estimate=pl.CostEstimate(
            flops=number * 6 * interior * interior * width,
            bytes_accessed=number * interior * (4 * interior + 4 * width),
            transcendentals=0,
        ),
        name="solve_half",
    )(half, factor, couple)


def tn(left, right):
    return lax.dot_general(left, right, (((0,), (0,)), ((), ())), preferred_element_type=F32)


def diagonal_kernel(slots_ref, send_ref, keep_ref, out_ref, sum_ref):
    step = pl.program_id(0)
    steps = pl.num_programs(0)
    groups = send_ref.shape[2] // BLK
    tiles = sum_ref.shape[0]

    @pl.when(step == 0)
    def _():
        sum_ref[...] = jnp.zeros_like(sum_ref)

    for which, ref in enumerate((send_ref, keep_ref)):
        for group in range(groups):
            columns = ref[0, :, group * BLK : (group + 1) * BLK]
            slot = slots_ref[which, step * groups + group]
            sum_ref[slot] += tn(columns, columns)

    @pl.when(step == steps - 1)
    def _():
        rows, cols = iotas(BLK, BLK)
        per_owner = tiles // out_ref.shape[0]

        def pack(owner, carry):
            lows = []
            for place in range(per_owner):
                value = sum_ref[owner * per_owner + place]
                high = value.astype(BF16).astype(F32)
                low = value - high
                packed = jnp.where(rows >= cols, high, low.T)
                out_ref[owner, place * BLK : (place + 1) * BLK, :] = packed.astype(BF16)
                lows.append(jnp.sum(jnp.where(rows == cols, low, 0.0), axis=0, keepdims=True))
            lows.append(jnp.zeros((EXTRA - per_owner, BLK), F32))
            out_ref[owner, per_owner * BLK :, :] = jnp.concatenate(lows, axis=0).astype(BF16)
            return carry

        lax.fori_loop(0, out_ref.shape[0], pack, 0)


def diagonal_sums(slots, send, keep, owner_count, places):
    number, interior, width = send.shape
    spec = pl.BlockSpec((1, interior, width), lambda i, slots: (i, 0, 0))
    rows = places * BLK + EXTRA
    return pl.pallas_call(
        diagonal_kernel,
        grid_spec=pltpu.PrefetchScalarGridSpec(
            num_scalar_prefetch=1,
            grid=(number,),
            in_specs=[spec, spec],
            out_specs=pl.BlockSpec((owner_count, rows, BLK), lambda i, slots: (0, 0, 0)),
            scratch_shapes=[pltpu.VMEM((owner_count * places, BLK, BLK), F32)],
        ),
        out_shape=jax.ShapeDtypeStruct((owner_count, rows, BLK), BF16),
        compiler_params=pltpu.CompilerParams(vmem_limit_bytes=VMEM_LIMIT),
        cost_estimate=pl.CostEstimate(
            flops=number * 8 * interior * width * BLK,
            bytes_accessed=number * interior * 4 * width,
            transcendentals=0,
        ),
        name="diagonal_sums",
    )(slots, send, keep)


def cross_kernel(slots_ref, linked_ref, keep_ref, partner_ref, out_ref, sum_ref):
    step = pl.program_id(0)
    steps = pl.num_programs(0)
    groups = keep_ref.shape[2] // BLK

    @pl.when(step == 0)
    def _():
        sum_ref[...] = jnp.zeros_like(sum_ref)

    for group in range(groups):
        span = slice(group * BLK, (group + 1) * BLK)
        product = tn(keep_ref[0, :, span], partner_ref[0, :, span])
        at = step * groups + group
        sum_ref[slots_ref[at]] += product * linked_ref[at].astype(F32)

    @pl.when(step == steps - 1)
    def _():
        out_ref[...] = sum_ref[...].astype(BF16)


def cross_sums(slots, linked, keep, partner, tiles):
    number, interior, width = keep.shape
    spec = pl.BlockSpec((1, interior, width), lambda i, slots, linked: (i, 0, 0))
    return pl.pallas_call(
        cross_kernel,
        grid_spec=pltpu.PrefetchScalarGridSpec(
            num_scalar_prefetch=2,
            grid=(number,),
            in_specs=[spec, spec],
            out_specs=pl.BlockSpec((tiles, BLK, BLK), lambda i, slots, linked: (0, 0, 0)),
            scratch_shapes=[pltpu.VMEM((tiles, BLK, BLK), F32)],
        ),
        out_shape=jax.ShapeDtypeStruct((tiles, BLK, BLK), BF16),
        compiler_params=pltpu.CompilerParams(vmem_limit_bytes=VMEM_LIMIT),
        cost_estimate=pl.CostEstimate(
            flops=number * 2 * interior * width * BLK,
            bytes_accessed=number * interior * 4 * width,
            transcendentals=0,
        ),
        name="cross_sums",
    )(slots, linked, keep, partner)


def exchange(value):
    count = lax.axis_size("panel")
    pairs = [(source, (source + count // 2) % count) for source in range(count)]
    return lax.ppermute(value, "panel", pairs)


def all_to_all(value):
    return lax.all_to_all(value, "sub", split_axis=0, concat_axis=0, tiled=True)


def per_device(
    interior_factor, coupling, interface_diag, interface_column, block_map, pair_pattern
):
    sub_count = lax.axis_size("sub")
    panel_count = lax.axis_size("panel")
    sub_index = lax.axis_index("sub")
    panel_index = lax.axis_index("panel")
    sub_local = coupling.shape[0]
    local_blocks = block_map.shape[1]
    groups = local_blocks // panel_count
    pair_offset = local_blocks // 2
    panel_rows = OWN // panel_count
    number = sub_local // 2
    upper = panel_index >= panel_count // 2
    other_index = (panel_index + panel_count // 2) % panel_count
    keep_half = upper.astype(jnp.int32)
    send_half = 1 - keep_half

    my_map = lax.dynamic_slice_in_dim(block_map, sub_index * sub_local, sub_local, 0)
    own_map = lax.dynamic_slice_in_dim(my_map, panel_index * groups, groups, 1)
    other_map = lax.dynamic_slice_in_dim(my_map, other_index * groups, groups, 1)
    places = own_map % OWN - panel_index * panel_rows
    other_places = other_map % OWN - other_index * panel_rows
    diagonal_slots = (own_map // OWN) * panel_rows + places
    cross_slots = diagonal_slots * panel_rows + other_places
    diagonal_slots = diagonal_slots.reshape(2, number * groups)
    diagonal_slots = jnp.where(upper, diagonal_slots, diagonal_slots[::-1])
    cross_slots = lax.dynamic_slice_in_dim(cross_slots, keep_half * number, number, 0).reshape(-1)
    pair_first = (panel_index * groups) % pair_offset
    linked = lax.dynamic_slice(
        pair_pattern, (keep_half * number, pair_first), (number, groups)
    ).reshape(-1)

    send = solve_half(send_half.reshape(1), interior_factor, coupling)
    partner = exchange(send)
    keep = solve_half(keep_half.reshape(1), interior_factor, coupling)
    diagonal = diagonal_sums(diagonal_slots, send, keep, sub_count, panel_rows)
    diagonal = all_to_all(diagonal)
    cross = cross_sums(cross_slots, linked, keep, partner, sub_count * panel_rows * panel_rows)
    cross = all_to_all(cross.reshape(sub_count, panel_rows * panel_rows * BLK, BLK))

    packed = jnp.sum(diagonal.astype(F32), axis=0)
    tail = packed[panel_rows * BLK : panel_rows * BLK + panel_rows]
    packed = packed[: panel_rows * BLK].reshape(panel_rows, BLK, BLK)
    eye = jnp.eye(BLK, dtype=F32)[None]
    extra = tail + interface_diag.reshape(panel_rows, BLK)
    square = packed + packed.transpose(0, 2, 1) * (1.0 - eye) + extra[:, None, :] * eye

    mine = jnp.sum(cross.astype(F32), axis=0).reshape(panel_rows, panel_rows, BLK, BLK)
    theirs = exchange(mine)
    full_cross = mine + theirs.transpose(1, 0, 3, 2)

    column = interface_column.reshape(panel_rows, BLK, BLK)
    is_pivot = jnp.logical_and(panel_index == 0, jnp.arange(panel_rows) == 0)
    own_part = jnp.where(is_pivot[:, None, None], square[:1], column)
    opposite = panel_index == panel_count // 2
    own_part = own_part + jnp.where(opposite, mine[:, 0], 0.0)
    across = mine[0].transpose(0, 2, 1)
    gathered = lax.all_gather(jnp.concatenate([own_part, across], axis=0), "panel", axis=0)
    whole = gathered[:, :panel_rows]
    whole = whole.at[panel_count // 2].add(gathered[0, panel_rows:])
    whole_column = whole.reshape(OWN * BLK, BLK)

    pivot = jnp.linalg.cholesky(whole_column[:BLK])
    lower_all = lax.linalg.triangular_solve(
        pivot, whole_column.T, left_side=True, lower=True
    ).T
    lower_all = jnp.concatenate([pivot, lower_all[BLK:]], axis=0)
    lower_own = lax.dynamic_slice_in_dim(
        lower_all, panel_index * panel_rows * BLK, panel_rows * BLK, 0
    )
    own_column = lax.dynamic_slice_in_dim(
        whole_column, panel_index * panel_rows * BLK, panel_rows * BLK, 0
    )
    update = jnp.einsum("ik,jk->ij", lower_own, lower_all, precision=lax.Precision.HIGHEST)

    rows = []
    for row in range(panel_rows):
        tiles = []
        for col in range(OWN):
            home, place = divmod(col, panel_rows)
            tile = jnp.where(other_index == home, full_cross[row, place], 0.0)
            if place == row:
                tile = jnp.where(panel_index == home, square[row], tile)
            if col == 0:
                tile = own_column[row * BLK : (row + 1) * BLK]
            tiles.append(tile)
        rows.append(jnp.concatenate(tiles, axis=1))
    assembled = jnp.concatenate(rows, axis=0)
    row_ids = jnp.arange(panel_rows * BLK, dtype=jnp.int32)[:, None]
    pivot_rows = jnp.logical_and(panel_index == 0, row_ids < BLK)
    updated = jnp.where(pivot_rows, assembled, assembled - update)
    factored = jnp.concatenate([lower_own, updated[:, BLK:]], axis=1)
    return (assembled, factored)


def solution(mesh):
    return jax.shard_map(
        per_device,
        mesh=mesh,
        in_specs=(
            P("sub", None, None),
            P("sub", None, "panel"),
            P(("sub", "panel")),
            P(("sub", "panel"), None),
            P(),
            P("sub", None),
        ),
        out_specs=(P(("sub", "panel"), None), P(("sub", "panel"), None)),
        check_vma=False,
    )
```

```python
import functools

import jax
import jax.numpy as jnp
from jax import lax
from jax.experimental import pallas as pl
from jax.experimental.pallas import tpu as pltpu
from jax.sharding import PartitionSpec as P

BLK = 128
OWN = 8
BASE = 32
EXTRA = 16
F32 = jnp.float32
BF16 = jnp.bfloat16
VMEM_LIMIT = 60 * 1024 * 1024


def halves(value):
    high = value.astype(BF16)
    return high, (value - high.astype(F32)).astype(BF16)


def mm(left, right):
    return jnp.dot(left, right, preferred_element_type=F32)


def mm_split(left, right):
    lh, ll = left
    rh, rl = right
    return mm(lh, rh) + (mm(lh, rl) + mm(ll, rh))


def iotas(rows, cols):
    return (
        lax.broadcasted_iota(jnp.int32, (rows, cols), 0),
        lax.broadcasted_iota(jnp.int32, (rows, cols), 1),
    )


def diagonal_inverse(block):
    row8, lane8 = iotas(8, BLK)
    group8 = lane8 // BASE
    within8 = lane8 - group8 * BASE
    tiles = BASE // 8
    rows, cols = iotas(BLK, BLK)
    side = []
    for tile in range(tiles):
        total = jnp.zeros((8, BLK), F32)
        for part in range(BLK // BASE):
            first = part * BASE + tile * 8
            total = jnp.where(group8 == part, block[first : first + 8, :], total)
        side.append(total)
    inverse = [jnp.where(within8 == row8 + tile * 8, 1.0, 0.0).astype(F32) for tile in range(tiles)]
    for step in range(BASE):
        at = step // 8
        inner = step % 8
        lanes = group8 * BASE + step
        spread = {
            tile: jnp.take_along_axis(side[tile], lanes, axis=1, mode="promise_in_bounds")
            for tile in range(at, tiles)
        }
        pivot_row = inverse[at][inner : inner + 1, :] / spread[at][inner : inner + 1, :]
        solved = jnp.broadcast_to(pivot_row, (8, BLK))
        lower = jnp.where(row8 > inner, inverse[at] - spread[at] * solved, inverse[at])
        inverse[at] = jnp.where(row8 == inner, solved, lower)
        for tile in range(at + 1, tiles):
            inverse[tile] = inverse[tile] - spread[tile] * solved
    stacked = jnp.concatenate(inverse * (BLK // BASE), axis=0)
    whole = jnp.where(rows // BASE == cols // BASE, stacked, 0.0)
    size = BASE
    while size < BLK:
        pair = 2 * size
        off = jnp.logical_and(
            rows // pair == cols // pair,
            jnp.logical_and(rows % pair >= size, cols % pair < size),
        )
        split = halves(whole)
        inner_product = mm_split(halves(jnp.where(off, block, 0.0)), split)
        whole = whole - mm_split(split, halves(inner_product))
        size = pair
    return whole


def solve_kernel(half_ref, factor_ref, couple_ref, out_ref, rest_ref):
    count, interior, width = couple_ref.shape
    total = interior // BLK
    inverses = [
        [
            halves(diagonal_inverse(factor_ref[item, b * BLK : (b + 1) * BLK, b * BLK : (b + 1) * BLK]))
            for b in range(total)
        ]
        for item in range(count)
    ]
    for b in range(total):
        for item in range(count):
            low = b * BLK
            inv_high, inv_low = inverses[item][b]
            if b == 0:
                right = couple_ref[item, 0:BLK, :]
                solved = mm(inv_high, right) + mm(inv_low, right)
            else:
                right = halves(rest_ref[item, low : low + BLK, :])
                solved = mm_split((inv_high, inv_low), right)
            out_ref[item, low : low + BLK, :] = solved.astype(BF16)
            if b + 1 < total:
                strip = halves(factor_ref[item, low + BLK :, low : low + BLK])
                update = mm_split(strip, halves(solved))
                if b == 0:
                    before = couple_ref[item, low + BLK :, :].astype(F32)
                else:
                    before = rest_ref[item, low + BLK :, :]
                rest_ref[item, low + BLK :, :] = before - update


def solve_some(start, count, factor, couple, weight):
    sub_local, interior, width = couple.shape
    return pl.pallas_call(
        solve_kernel,
        grid_spec=pltpu.PrefetchScalarGridSpec(
            num_scalar_prefetch=1,
            grid=(count,),
            in_specs=[
                pl.BlockSpec((1, interior, interior), lambda i, start: (start[0] + i, 0, 0)),
                pl.BlockSpec((1, interior, width), lambda i, start: (start[0] + i, 0, 0)),
            ],
            out_specs=pl.BlockSpec((1, interior, width), lambda i, start: (i, 0, 0)),
            scratch_shapes=[pltpu.VMEM((1, interior, width), F32)],
        ),
        out_shape=jax.ShapeDtypeStruct((count, interior, width), BF16),
        compiler_params=pltpu.CompilerParams(vmem_limit_bytes=VMEM_LIMIT),
        cost_estimate=pl.CostEstimate(
            flops=weight * count * interior * interior * width,
            bytes_accessed=weight * count * interior * BLK,
            transcendentals=0,
        ),
        name="solve_some",
    )(start.reshape(1), factor, couple)


def tn(left, right):
    return lax.dot_general(left, right, (((0,), (0,)), ((), ())), preferred_element_type=F32)


def diagonal_kernel(slots_ref, send_ref, keep_ref, out_ref, sum_ref):
    step = pl.program_id(0)
    steps = pl.num_programs(0)
    groups = send_ref.shape[2] // BLK
    tiles = sum_ref.shape[0]

    @pl.when(step == 0)
    def _():
        sum_ref[...] = jnp.zeros_like(sum_ref)

    for which, ref in enumerate((send_ref, keep_ref)):
        for group in range(groups):
            columns = ref[0, :, group * BLK : (group + 1) * BLK]
            slot = slots_ref[which, step * groups + group]
            sum_ref[slot] += tn(columns, columns)

    @pl.when(step == steps - 1)
    def _():
        rows, cols = iotas(BLK, BLK)
        per_owner = tiles // out_ref.shape[0]

        def pack(owner, carry):
            lows = []
            for place in range(per_owner):
                value = sum_ref[owner * per_owner + place]
                high = value.astype(BF16).astype(F32)
                low = value - high
                packed = jnp.where(rows >= cols, high, low.T)
                out_ref[owner, place * BLK : (place + 1) * BLK, :] = packed.astype(BF16)
                lows.append(jnp.sum(jnp.where(rows == cols, low, 0.0), axis=0, keepdims=True))
            lows.append(jnp.zeros((EXTRA - per_owner, BLK), F32))
            out_ref[owner, per_owner * BLK :, :] = jnp.concatenate(lows, axis=0).astype(BF16)
            return carry

        lax.fori_loop(0, out_ref.shape[0], pack, 0)


def diagonal_sums(slots, send, keep, owner_count, places):
    number, interior, width = send.shape
    spec = pl.BlockSpec((1, interior, width), lambda i, slots: (i, 0, 0))
    rows = places * BLK + EXTRA
    return pl.pallas_call(
        diagonal_kernel,
        grid_spec=pltpu.PrefetchScalarGridSpec(
            num_scalar_prefetch=1,
            grid=(number,),
            in_specs=[spec, spec],
            out_specs=pl.BlockSpec((owner_count, rows, BLK), lambda i, slots: (0, 0, 0)),
            scratch_shapes=[pltpu.VMEM((owner_count * places, BLK, BLK), F32)],
        ),
        out_shape=jax.ShapeDtypeStruct((owner_count, rows, BLK), BF16),
        compiler_params=pltpu.CompilerParams(vmem_limit_bytes=VMEM_LIMIT),
        cost_estimate=pl.CostEstimate(
            flops=number * interior * width,
            bytes_accessed=number * interior * BLK,
            transcendentals=0,
        ),
        name="diagonal_sums",
    )(slots, send, keep)


def cross_kernel(first, last, offset, slots_ref, linked_ref, keep_ref, partner_ref, *refs):
    out_ref, sum_ref = refs[-2:]
    step = pl.program_id(0)
    groups = keep_ref.shape[2] // BLK

    @pl.when(step == 0)
    def _():
        sum_ref[...] = jnp.zeros_like(sum_ref) if first else refs[0][...]

    for group in range(groups):
        span = slice(group * BLK, (group + 1) * BLK)
        product = tn(keep_ref[0, :, span], partner_ref[0, :, span])
        at = (step + offset) * groups + group
        sum_ref[slots_ref[at]] += product * linked_ref[at].astype(F32)

    @pl.when(step == pl.num_programs(0) - 1)
    def _():
        out_ref[...] = sum_ref[...].astype(out_ref.dtype)


def cross_sums(slots, linked, keep, partner, offset, before, tiles):
    number, interior, width = keep.shape
    count = partner.shape[0]
    first, last = offset == 0, offset + count == number
    whole = pl.BlockSpec((tiles, BLK, BLK), lambda i, slots, linked: (0, 0, 0))
    dtype = BF16 if last else F32
    return pl.pallas_call(
        functools.partial(cross_kernel, first, last, offset),
        grid_spec=pltpu.PrefetchScalarGridSpec(
            num_scalar_prefetch=2,
            grid=(count,),
            in_specs=[
                pl.BlockSpec((1, interior, width), lambda i, slots, linked: (i + offset, 0, 0)),
                pl.BlockSpec((1, interior, width), lambda i, slots, linked: (i, 0, 0)),
            ]
            + ([] if first else [whole]),
            out_specs=whole,
            scratch_shapes=[pltpu.VMEM((tiles, BLK, BLK), F32)],
        ),
        out_shape=jax.ShapeDtypeStruct((tiles, BLK, BLK), dtype),
        compiler_params=pltpu.CompilerParams(vmem_limit_bytes=VMEM_LIMIT),
        cost_estimate=pl.CostEstimate(
            flops=count * 2 * interior * width * BLK,
            bytes_accessed=count * interior * 4 * width,
            transcendentals=0,
        ),
        name="cross_sums",
    )(slots, linked, keep, partner, *([] if first else [before]))


def factor_pivot(block):
    row8, lane8 = iotas(8, BLK)
    rows, cols = iotas(BLK, BLK)
    tiles = BLK // 8
    upper = [block[t * 8 : (t + 1) * 8, :] for t in range(tiles)]
    carried = [jnp.where(lane8 == row8 + t * 8, 1.0, 0.0).astype(F32) for t in range(tiles)]
    scales = []
    for at in range(tiles):
        spread = [
            {
                t: jnp.broadcast_to(upper[t][:, at * 8 + i : at * 8 + i + 1], (8, BLK))
                for t in range(at, tiles)
            }
            for i in range(8)
        ]
        scale = jnp.zeros((8, BLK), F32)
        for i in range(8):
            pivot = jnp.broadcast_to(spread[i][at][i : i + 1, :], (8, BLK))
            scale = jnp.where(row8 == i, lax.rsqrt(pivot), scale)
            inverse = 1.0 / pivot
            upper_row = jnp.broadcast_to(upper[at][i : i + 1, :], (8, BLK))
            carried_row = jnp.broadcast_to(carried[at][i : i + 1, :], (8, BLK))
            later = {
                j: jnp.broadcast_to(spread[j][at][i : i + 1, :], (8, BLK)) for j in range(i + 1, 8)
            }
            for t in range(at, tiles):
                ratio = spread[i][t] * inverse
                if t == at:
                    ratio = jnp.where(row8 > i, ratio, 0.0)
                upper[t] = upper[t] - ratio * upper_row
                carried[t] = carried[t] - ratio * carried_row
                for j in range(i + 1, 8):
                    spread[j][t] = spread[j][t] - ratio * later[j]
        scales.append(scale)
    scale = jnp.concatenate(scales, axis=0)
    upper = jnp.concatenate(upper, axis=0) * scale
    carried = jnp.concatenate(carried, axis=0) * scale
    factor = jnp.where(rows <= cols, upper, 0.0).T
    return factor, jnp.where(rows >= cols, carried, 0.0)


def nt(left, right):
    return lax.dot_general(left, right, (((1,), (1,)), ((), ())), preferred_element_type=F32)


def nt_split(left, right):
    lh, ll = left
    rh, rl = right
    return nt(lh, rh) + (nt(lh, rl) + nt(ll, rh))


def tail_kernel(
    panel_count, panel_ref, column_ref, square_ref, mine_ref, theirs_ref, out_ref, done_ref, low_ref
):
    panel = panel_ref[0]
    other = lax.rem(panel + panel_count // 2, panel_count)
    panel_rows = square_ref.shape[0]
    factor, inverse = factor_pivot(column_ref[0:BLK, :])
    low_ref[0:BLK, :] = factor
    low_ref[BLK:, :] = nt_split(halves(column_ref[BLK:, :]), halves(inverse))
    start = pl.multiple_of(panel * (panel_rows * BLK), panel_rows * BLK)
    own = low_ref[pl.ds(start, panel_rows * BLK), :]
    own_column = column_ref[pl.ds(start, panel_rows * BLK), :]
    own_split = halves(own)
    out_ref[:, 0:BLK] = own_column
    done_ref[:, 0:BLK] = own
    crosses = [
        [mine_ref[row, place] + theirs_ref[place, row].T for place in range(panel_rows)]
        for row in range(panel_rows)
    ]
    for col in range(1, OWN):
        home, place = divmod(col, panel_rows)
        update = nt_split(own_split, halves(low_ref[col * BLK : (col + 1) * BLK, :]))
        for row in range(panel_rows):
            tile = jnp.where(other == home, crosses[row][place], 0.0)
            if place == row:
                tile = jnp.where(panel == home, square_ref[row], tile)
            part = update[row * BLK : (row + 1) * BLK, :]
            if row == 0:
                part = jnp.where(panel == 0, 0.0, part)
            span = slice(col * BLK, (col + 1) * BLK)
            out_ref[row * BLK : (row + 1) * BLK, span] = tile
            done_ref[row * BLK : (row + 1) * BLK, span] = tile - part


def finish(panel_count, panel_index, column, square, mine, theirs):
    panel_rows = square.shape[0]
    shape = jax.ShapeDtypeStruct((panel_rows * BLK, OWN * BLK), F32)
    vmem = pl.BlockSpec(memory_space=pltpu.VMEM)
    return pl.pallas_call(
        functools.partial(tail_kernel, panel_count),
        in_specs=[pl.BlockSpec(memory_space=pltpu.SMEM)] + [vmem] * 4,
        out_specs=[vmem, vmem],
        out_shape=[shape, shape],
        scratch_shapes=[pltpu.VMEM((OWN * BLK, BLK), F32)],
        compiler_params=pltpu.CompilerParams(vmem_limit_bytes=VMEM_LIMIT),
        name="tail",
    )(panel_index.reshape(1), column, square, mine, theirs)


def exchange(value):
    count = lax.axis_size("panel")
    pairs = [(source, (source + count // 2) % count) for source in range(count)]
    return lax.ppermute(value, "panel", pairs)


def all_to_all(value):
    return lax.all_to_all(value, "sub", split_axis=0, concat_axis=0, tiled=True)


def per_device(
    interior_factor, coupling, interface_diag, interface_column, block_map, pair_pattern
):
    sub_count = lax.axis_size("sub")
    panel_count = lax.axis_size("panel")
    sub_index = lax.axis_index("sub")
    panel_index = lax.axis_index("panel")
    sub_local = coupling.shape[0]
    local_blocks = block_map.shape[1]
    groups = local_blocks // panel_count
    pair_offset = local_blocks // 2
    panel_rows = OWN // panel_count
    number = sub_local // 2
    upper = panel_index >= panel_count // 2
    other_index = (panel_index + panel_count // 2) % panel_count
    keep_half = upper.astype(jnp.int32)
    send_half = 1 - keep_half

    my_map = lax.dynamic_slice_in_dim(block_map, sub_index * sub_local, sub_local, 0)
    own_map = lax.dynamic_slice_in_dim(my_map, panel_index * groups, groups, 1)
    other_map = lax.dynamic_slice_in_dim(my_map, other_index * groups, groups, 1)
    places = own_map % OWN - panel_index * panel_rows
    other_places = other_map % OWN - other_index * panel_rows
    diagonal_slots = (own_map // OWN) * panel_rows + places
    cross_slots = diagonal_slots * panel_rows + other_places
    diagonal_slots = diagonal_slots.reshape(2, number * groups)
    diagonal_slots = jnp.where(upper, diagonal_slots, diagonal_slots[::-1])
    cross_slots = lax.dynamic_slice_in_dim(cross_slots, keep_half * number, number, 0).reshape(-1)
    pair_first = (panel_index * groups) % pair_offset
    linked = lax.dynamic_slice(
        pair_pattern, (keep_half * number, pair_first), (number, groups)
    ).reshape(-1)

    counts = [number // 2, number - number // 2] if number > 1 else [number]
    sends, partners, offset = [], [], 0
    for count in counts:
        start = send_half * number + offset
        if sends:
            start, _ = lax.optimization_barrier((start, sends[-1]))
        solved = solve_some(start, count, interior_factor, coupling, 16)
        sends.append(solved)
        partners.append(exchange(solved))
        offset += count
    start, _ = lax.optimization_barrier((keep_half * number, sends[-1]))
    keep = solve_some(start, number, interior_factor, coupling, 1)
    send = jnp.concatenate(sends, axis=0)
    diagonal = diagonal_sums(diagonal_slots, send, keep, sub_count, panel_rows)
    diagonal = all_to_all(diagonal)
    cross, offset = None, 0
    for partner in partners:
        cross = cross_sums(
            cross_slots, linked, keep, partner, offset, cross, sub_count * panel_rows * panel_rows
        )
        offset += partner.shape[0]
    cross = all_to_all(cross.reshape(sub_count, panel_rows * panel_rows * BLK, BLK))

    packed = jnp.sum(diagonal.astype(F32), axis=0)
    low_diag = packed[panel_rows * BLK : panel_rows * BLK + panel_rows]
    packed = packed[: panel_rows * BLK].reshape(panel_rows, BLK, BLK)
    eye = jnp.eye(BLK, dtype=F32)[None]
    extra = low_diag + interface_diag.reshape(panel_rows, BLK)
    square = packed + packed.transpose(0, 2, 1) * (1.0 - eye) + extra[:, None, :] * eye

    mine = jnp.sum(cross.astype(F32), axis=0).reshape(panel_rows, panel_rows, BLK, BLK)
    theirs = exchange(mine)

    column = interface_column.reshape(panel_rows, BLK, BLK)
    is_pivot = jnp.logical_and(panel_index == 0, jnp.arange(panel_rows) == 0)
    own_part = jnp.where(is_pivot[:, None, None], square[:1], column)
    opposite = panel_index == panel_count // 2
    own_part = own_part + jnp.where(opposite, mine[:, 0], 0.0)
    across = mine[0].transpose(0, 2, 1)
    gathered = lax.all_gather(jnp.concatenate([own_part, across], axis=0), "panel", axis=0)
    whole = gathered[:, :panel_rows]
    whole = whole.at[panel_count // 2].add(gathered[0, panel_rows:])
    whole_column = whole.reshape(OWN * BLK, BLK)

    return tuple(finish(panel_count, panel_index, whole_column, square, mine, theirs))


def solution(mesh):
    return jax.shard_map(
        per_device,
        mesh=mesh,
        in_specs=(
            P("sub", None, None),
            P("sub", None, "panel"),
            P(("sub", "panel")),
            P(("sub", "panel"), None),
            P(),
            P("sub", None),
        ),
        out_specs=(P(("sub", "panel"), None), P(("sub", "panel"), None)),
        check_vma=False,
    )
```

```python
import functools

import jax
import jax.numpy as jnp
from jax import lax
from jax.experimental import pallas as pl
from jax.experimental.pallas import tpu as pltpu
from jax.sharding import PartitionSpec as P

BLK = 128
OWN = 8
BASE = 32
EXTRA = 16
F32 = jnp.float32
BF16 = jnp.bfloat16
VMEM_LIMIT = 60 * 1024 * 1024


def halves(value):
    high = value.astype(BF16)
    return high, (value - high.astype(F32)).astype(BF16)


def mm(left, right):
    return jnp.dot(left, right, preferred_element_type=F32)


def mm_split(left, right):
    lh, ll = left
    rh, rl = right
    return mm(lh, rh) + (mm(lh, rl) + mm(ll, rh))


def iotas(rows, cols):
    return (
        lax.broadcasted_iota(jnp.int32, (rows, cols), 0),
        lax.broadcasted_iota(jnp.int32, (rows, cols), 1),
    )


def diagonal_inverse(block):
    row8, lane8 = iotas(8, BLK)
    group8 = lane8 // BASE
    within8 = lane8 - group8 * BASE
    tiles = BASE // 8
    rows, cols = iotas(BLK, BLK)
    side = []
    for tile in range(tiles):
        total = jnp.zeros((8, BLK), F32)
        for part in range(BLK // BASE):
            first = part * BASE + tile * 8
            total = jnp.where(group8 == part, block[first : first + 8, :], total)
        side.append(total)
    inverse = [jnp.where(within8 == row8 + tile * 8, 1.0, 0.0).astype(F32) for tile in range(tiles)]
    for step in range(BASE):
        at = step // 8
        inner = step % 8
        lanes = group8 * BASE + step
        spread = {
            tile: jnp.take_along_axis(side[tile], lanes, axis=1, mode="promise_in_bounds")
            for tile in range(at, tiles)
        }
        pivot_row = inverse[at][inner : inner + 1, :] / spread[at][inner : inner + 1, :]
        solved = jnp.broadcast_to(pivot_row, (8, BLK))
        lower = jnp.where(row8 > inner, inverse[at] - spread[at] * solved, inverse[at])
        inverse[at] = jnp.where(row8 == inner, solved, lower)
        for tile in range(at + 1, tiles):
            inverse[tile] = inverse[tile] - spread[tile] * solved
    stacked = jnp.concatenate(inverse * (BLK // BASE), axis=0)
    whole = jnp.where(rows // BASE == cols // BASE, stacked, 0.0)
    size = BASE
    while size < BLK:
        pair = 2 * size
        off = jnp.logical_and(
            rows // pair == cols // pair,
            jnp.logical_and(rows % pair >= size, cols % pair < size),
        )
        split = halves(whole)
        inner_product = mm_split(halves(jnp.where(off, block, 0.0)), split)
        whole = whole - mm_split(split, halves(inner_product))
        size = pair
    return whole


def solve_kernel(half_ref, factor_ref, couple_ref, out_ref, rest_ref):
    count, interior, width = couple_ref.shape
    total = interior // BLK
    inverses = [
        [
            halves(diagonal_inverse(factor_ref[item, b * BLK : (b + 1) * BLK, b * BLK : (b + 1) * BLK]))
            for b in range(total)
        ]
        for item in range(count)
    ]
    for b in range(total):
        for item in range(count):
            low = b * BLK
            inv_high, inv_low = inverses[item][b]
            if b == 0:
                right = couple_ref[item, 0:BLK, :]
                solved = mm(inv_high, right) + mm(inv_low, right)
            else:
                right = halves(rest_ref[item, low : low + BLK, :])
                solved = mm_split((inv_high, inv_low), right)
            out_ref[item, low : low + BLK, :] = solved.astype(BF16)
            if b + 1 < total:
                strip = halves(factor_ref[item, low + BLK :, low : low + BLK])
                update = mm_split(strip, halves(solved))
                if b == 0:
                    before = couple_ref[item, low + BLK :, :].astype(F32)
                else:
                    before = rest_ref[item, low + BLK :, :]
                rest_ref[item, low + BLK :, :] = before - update


def solve_some(start, count, factor, couple, weight):
    sub_local, interior, width = couple.shape
    return pl.pallas_call(
        solve_kernel,
        grid_spec=pltpu.PrefetchScalarGridSpec(
            num_scalar_prefetch=1,
            grid=(count,),
            in_specs=[
                pl.BlockSpec((1, interior, interior), lambda i, start: (start[0] + i, 0, 0)),
                pl.BlockSpec((1, interior, width), lambda i, start: (start[0] + i, 0, 0)),
            ],
            out_specs=pl.BlockSpec((1, interior, width), lambda i, start: (i, 0, 0)),
            scratch_shapes=[pltpu.VMEM((1, interior, width), F32)],
        ),
        out_shape=jax.ShapeDtypeStruct((count, interior, width), BF16),
        compiler_params=pltpu.CompilerParams(vmem_limit_bytes=VMEM_LIMIT),
        cost_estimate=pl.CostEstimate(
            flops=weight * count * interior * interior * width,
            bytes_accessed=weight * count * interior * BLK,
            transcendentals=0,
        ),
        name="solve_some",
    )(start.reshape(1), factor, couple)


def tn(left, right):
    return lax.dot_general(left, right, (((0,), (0,)), ((), ())), preferred_element_type=F32)


def diagonal_kernel(slots_ref, send_ref, keep_ref, out_ref, sum_ref):
    step = pl.program_id(0)
    steps = pl.num_programs(0)
    groups = send_ref.shape[2] // BLK
    tiles = sum_ref.shape[0]

    @pl.when(step == 0)
    def _():
        sum_ref[...] = jnp.zeros_like(sum_ref)

    for which, ref in enumerate((send_ref, keep_ref)):
        for group in range(groups):
            columns = ref[0, :, group * BLK : (group + 1) * BLK]
            slot = slots_ref[which, step * groups + group]
            sum_ref[slot] += tn(columns, columns)

    @pl.when(step == steps - 1)
    def _():
        rows, cols = iotas(BLK, BLK)
        per_owner = tiles // out_ref.shape[0]

        def pack(owner, carry):
            lows = []
            for place in range(per_owner):
                value = sum_ref[owner * per_owner + place]
                high = value.astype(BF16).astype(F32)
                low = value - high
                packed = jnp.where(rows >= cols, high, low.T)
                out_ref[owner, place * BLK : (place + 1) * BLK, :] = packed.astype(BF16)
                lows.append(jnp.sum(jnp.where(rows == cols, low, 0.0), axis=0, keepdims=True))
            lows.append(jnp.zeros((EXTRA - per_owner, BLK), F32))
            out_ref[owner, per_owner * BLK :, :] = jnp.concatenate(lows, axis=0).astype(BF16)
            return carry

        lax.fori_loop(0, out_ref.shape[0], pack, 0)


def diagonal_sums(slots, send, keep, owner_count, places):
    number, interior, width = send.shape
    spec = pl.BlockSpec((1, interior, width), lambda i, slots: (i, 0, 0))
    rows = places * BLK + EXTRA
    return pl.pallas_call(
        diagonal_kernel,
        grid_spec=pltpu.PrefetchScalarGridSpec(
            num_scalar_prefetch=1,
            grid=(number,),
            in_specs=[spec, spec],
            out_specs=pl.BlockSpec((owner_count, rows, BLK), lambda i, slots: (0, 0, 0)),
            scratch_shapes=[pltpu.VMEM((owner_count * places, BLK, BLK), F32)],
        ),
        out_shape=jax.ShapeDtypeStruct((owner_count, rows, BLK), BF16),
        compiler_params=pltpu.CompilerParams(vmem_limit_bytes=VMEM_LIMIT),
        cost_estimate=pl.CostEstimate(
            flops=number * interior * width,
            bytes_accessed=number * interior * BLK,
            transcendentals=0,
        ),
        name="diagonal_sums",
    )(slots, send, keep)


def cross_kernel(chunks, slots_ref, linked_ref, *refs):
    out_ref, sum_ref = refs[-2:]
    step = pl.program_id(0)
    steps = pl.num_programs(0)
    groups = refs[0].shape[2] // BLK

    @pl.when(step == 0)
    def _():
        sum_ref[...] = jnp.zeros_like(sum_ref)

    for chunk in range(chunks):
        keep_ref, partner_ref = refs[2 * chunk : 2 * chunk + 2]
        for group in range(groups):
            span = slice(group * BLK, (group + 1) * BLK)
            product = tn(keep_ref[0, :, span], partner_ref[0, :, span])
            at = (chunk * steps + step) * groups + group
            sum_ref[slots_ref[at]] += product * linked_ref[at].astype(F32)

    @pl.when(step == steps - 1)
    def _():
        out_ref[...] = sum_ref[...].astype(out_ref.dtype)


def cross_sums(slots, linked, keep, partners, tiles):
    number, interior, width = keep.shape
    chunks = len(partners)
    steps = number // chunks
    specs, operands = [], []
    for chunk, partner in enumerate(partners):
        first = chunk * steps
        specs.append(
            pl.BlockSpec(
                (1, interior, width), lambda i, slots, linked, first=first: (i + first, 0, 0)
            )
        )
        specs.append(pl.BlockSpec((1, interior, width), lambda i, slots, linked: (i, 0, 0)))
        operands += [keep, partner]
    return pl.pallas_call(
        functools.partial(cross_kernel, chunks),
        grid_spec=pltpu.PrefetchScalarGridSpec(
            num_scalar_prefetch=2,
            grid=(steps,),
            in_specs=specs,
            out_specs=pl.BlockSpec((tiles, BLK, BLK), lambda i, slots, linked: (0, 0, 0)),
            scratch_shapes=[pltpu.VMEM((tiles, BLK, BLK), F32)],
        ),
        out_shape=jax.ShapeDtypeStruct((tiles, BLK, BLK), BF16),
        compiler_params=pltpu.CompilerParams(vmem_limit_bytes=VMEM_LIMIT),
        name="cross_sums",
    )(slots, linked, *operands)


def factor_pivot(block):
    row8, lane8 = iotas(8, BLK)
    rows, cols = iotas(BLK, BLK)
    tiles = BLK // 8
    upper = [block[t * 8 : (t + 1) * 8, :] for t in range(tiles)]
    carried = [jnp.where(lane8 == row8 + t * 8, 1.0, 0.0).astype(F32) for t in range(tiles)]
    scales = []
    for at in range(tiles):
        spread = [
            {
                t: jnp.broadcast_to(upper[t][:, at * 8 + i : at * 8 + i + 1], (8, BLK))
                for t in range(at, tiles)
            }
            for i in range(8)
        ]
        scale = jnp.zeros((8, BLK), F32)
        for i in range(8):
            pivot = jnp.broadcast_to(spread[i][at][i : i + 1, :], (8, BLK))
            scale = jnp.where(row8 == i, lax.rsqrt(pivot), scale)
            inverse = 1.0 / pivot
            upper_row = jnp.broadcast_to(upper[at][i : i + 1, :], (8, BLK))
            carried_row = jnp.broadcast_to(carried[at][i : i + 1, :], (8, BLK))
            later = {
                j: jnp.broadcast_to(spread[j][at][i : i + 1, :], (8, BLK)) for j in range(i + 1, 8)
            }
            for t in range(at, tiles):
                ratio = spread[i][t] * inverse
                if t == at:
                    ratio = jnp.where(row8 > i, ratio, 0.0)
                upper[t] = upper[t] - ratio * upper_row
                carried[t] = carried[t] - ratio * carried_row
                for j in range(i + 1, 8):
                    spread[j][t] = spread[j][t] - ratio * later[j]
        scales.append(scale)
    scale = jnp.concatenate(scales, axis=0)
    upper = jnp.concatenate(upper, axis=0) * scale
    carried = jnp.concatenate(carried, axis=0) * scale
    factor = jnp.where(rows <= cols, upper, 0.0).T
    return factor, jnp.where(rows >= cols, carried, 0.0)


def nt(left, right):
    return lax.dot_general(left, right, (((1,), (1,)), ((), ())), preferred_element_type=F32)


def nt_split(left, right):
    lh, ll = left
    rh, rl = right
    return nt(lh, rh) + (nt(lh, rl) + nt(ll, rh))


def tail_kernel(
    panel_count, panel_ref, column_ref, square_ref, mine_ref, theirs_ref, out_ref, done_ref, low_ref
):
    panel = panel_ref[0]
    other = lax.rem(panel + panel_count // 2, panel_count)
    panel_rows = square_ref.shape[0]
    factor, inverse = factor_pivot(column_ref[0:BLK, :])
    low_ref[0:BLK, :] = factor
    low_ref[BLK:, :] = nt_split(halves(column_ref[BLK:, :]), halves(inverse))
    start = pl.multiple_of(panel * (panel_rows * BLK), panel_rows * BLK)
    own = low_ref[pl.ds(start, panel_rows * BLK), :]
    own_column = column_ref[pl.ds(start, panel_rows * BLK), :]
    own_split = halves(own)
    out_ref[:, 0:BLK] = own_column
    done_ref[:, 0:BLK] = own
    crosses = [
        [mine_ref[row, place] + theirs_ref[place, row].T for place in range(panel_rows)]
        for row in range(panel_rows)
    ]
    for col in range(1, OWN):
        home, place = divmod(col, panel_rows)
        update = nt_split(own_split, halves(low_ref[col * BLK : (col + 1) * BLK, :]))
        for row in range(panel_rows):
            tile = jnp.where(other == home, crosses[row][place], 0.0)
            if place == row:
                tile = jnp.where(panel == home, square_ref[row], tile)
            part = update[row * BLK : (row + 1) * BLK, :]
            if row == 0:
                part = jnp.where(panel == 0, 0.0, part)
            span = slice(col * BLK, (col + 1) * BLK)
            out_ref[row * BLK : (row + 1) * BLK, span] = tile
            done_ref[row * BLK : (row + 1) * BLK, span] = tile - part


def finish(panel_count, panel_index, column, square, mine, theirs):
    panel_rows = square.shape[0]
    shape = jax.ShapeDtypeStruct((panel_rows * BLK, OWN * BLK), F32)
    vmem = pl.BlockSpec(memory_space=pltpu.VMEM)
    return pl.pallas_call(
        functools.partial(tail_kernel, panel_count),
        in_specs=[pl.BlockSpec(memory_space=pltpu.SMEM)] + [vmem] * 4,
        out_specs=[vmem, vmem],
        out_shape=[shape, shape],
        scratch_shapes=[pltpu.VMEM((OWN * BLK, BLK), F32)],
        compiler_params=pltpu.CompilerParams(vmem_limit_bytes=VMEM_LIMIT),
        name="tail",
    )(panel_index.reshape(1), column, square, mine, theirs)


def exchange(value):
    count = lax.axis_size("panel")
    pairs = [(source, (source + count // 2) % count) for source in range(count)]
    return lax.ppermute(value, "panel", pairs)


def all_to_all(value):
    return lax.all_to_all(value, "sub", split_axis=0, concat_axis=0, tiled=True)


def per_device(
    interior_factor, coupling, interface_diag, interface_column, block_map, pair_pattern
):
    sub_count = lax.axis_size("sub")
    panel_count = lax.axis_size("panel")
    sub_index = lax.axis_index("sub")
    panel_index = lax.axis_index("panel")
    sub_local = coupling.shape[0]
    local_blocks = block_map.shape[1]
    groups = local_blocks // panel_count
    pair_offset = local_blocks // 2
    panel_rows = OWN // panel_count
    number = sub_local // 2
    upper = panel_index >= panel_count // 2
    other_index = (panel_index + panel_count // 2) % panel_count
    keep_half = upper.astype(jnp.int32)
    send_half = 1 - keep_half

    my_map = lax.dynamic_slice_in_dim(block_map, sub_index * sub_local, sub_local, 0)
    own_map = lax.dynamic_slice_in_dim(my_map, panel_index * groups, groups, 1)
    other_map = lax.dynamic_slice_in_dim(my_map, other_index * groups, groups, 1)
    places = own_map % OWN - panel_index * panel_rows
    other_places = other_map % OWN - other_index * panel_rows
    diagonal_slots = (own_map // OWN) * panel_rows + places
    cross_slots = diagonal_slots * panel_rows + other_places
    diagonal_slots = diagonal_slots.reshape(2, number * groups)
    diagonal_slots = jnp.where(upper, diagonal_slots, diagonal_slots[::-1])
    cross_slots = lax.dynamic_slice_in_dim(cross_slots, keep_half * number, number, 0).reshape(-1)
    pair_first = (panel_index * groups) % pair_offset
    linked = lax.dynamic_slice(
        pair_pattern, (keep_half * number, pair_first), (number, groups)
    ).reshape(-1)

    counts = [number // 2] * 2 if number % 2 == 0 else [number]
    sends, partners, offset = [], [], 0
    for count in counts:
        start = send_half * number + offset
        if sends:
            start, _ = lax.optimization_barrier((start, sends[-1]))
        solved = solve_some(start, count, interior_factor, coupling, 16)
        sends.append(solved)
        partners.append(exchange(solved))
        offset += count
    start, _ = lax.optimization_barrier((keep_half * number, sends[-1]))
    keep = solve_some(start, number, interior_factor, coupling, 1)
    send = jnp.concatenate(sends, axis=0)
    diagonal = diagonal_sums(diagonal_slots, send, keep, sub_count, panel_rows)
    diagonal = all_to_all(diagonal)
    cross = cross_sums(
        cross_slots, linked, keep, partners, sub_count * panel_rows * panel_rows
    )
    cross = all_to_all(cross.reshape(sub_count, panel_rows * panel_rows * BLK, BLK))

    packed = jnp.sum(diagonal.astype(F32), axis=0)
    low_diag = packed[panel_rows * BLK : panel_rows * BLK + panel_rows]
    packed = packed[: panel_rows * BLK].reshape(panel_rows, BLK, BLK)
    eye = jnp.eye(BLK, dtype=F32)[None]
    extra = low_diag + interface_diag.reshape(panel_rows, BLK)
    square = packed + packed.transpose(0, 2, 1) * (1.0 - eye) + extra[:, None, :] * eye

    mine = jnp.sum(cross.astype(F32), axis=0).reshape(panel_rows, panel_rows, BLK, BLK)
    theirs = exchange(mine)

    column = interface_column.reshape(panel_rows, BLK, BLK)
    is_pivot = jnp.logical_and(panel_index == 0, jnp.arange(panel_rows) == 0)
    own_part = jnp.where(is_pivot[:, None, None], square[:1], column)
    opposite = panel_index == panel_count // 2
    full = mine[:, 0] + theirs[0].transpose(0, 2, 1)
    own_part = own_part + jnp.where(opposite, full, 0.0)
    gathered = lax.all_gather(
        own_part.reshape(panel_rows * BLK, BLK), "panel", axis=0, tiled=True
    )
    whole_column = gathered

    return tuple(finish(panel_count, panel_index, whole_column, square, mine, theirs))


def solution(mesh):
    return jax.shard_map(
        per_device,
        mesh=mesh,
        in_specs=(
            P("sub", None, None),
            P("sub", None, "panel"),
            P(("sub", "panel")),
            P(("sub", "panel"), None),
            P(),
            P("sub", None),
        ),
        out_specs=(P(("sub", "panel"), None), P(("sub", "panel"), None)),
        check_vma=False,
    )
```
